128 devices in a mesh: sub: 16 (over z_lo, y, core), pole: 8 (over x, z_hi).
Axes of the slice: x: 4, y: 4, z: 4 (z_hi: 2, z_lo: 2; z = z_hi * 2 + z_lo), core: 2. Of those that a mesh axis runs over, the one named last changes fastest.
Arguments:
- state: float32 [12288, 512], P('sub'), may hold values from -6 to 6
- conductivity: float32 [12288], P('sub'), may hold values from 0.2 to 2
- pole_shift: float32 [8, 2], P('pole'), may hold values from 0.2 to 1
- pole_weight: float32 [8, 2], P('pole'), may hold values from -1.5 to 1.5
- order_list: int32 [16, 1024], P('sub'), may hold values from 0 to 1023, as said below
- inverse: bfloat16 [8, 12288, 2048], P('pole', 'sub'), may hold values from -0.1 to 0.4
Outputs:
- final_state: float32 [12288, 512], P(('sub', 'pole'))
The draws below stay inside these ranges and needn't reach their ends.
Inputs may be any that keep to these rules, and one draw needn't show every extreme that they name: `order_list`: row s holds each of 0 to 1023 exactly once.
All inputs are finite; a program needn't handle non-finite values.
Results may differ from the reference program's by a relative error of at most 0.0052.
Values may be sent and summed in bfloat16 or wider, within the bound.
A program may use at most 64 MiB of HBM per device.

```python
import math
import jax
import jax.numpy as jnp
from jax import lax

ORDER = 1024
H = 128
SRC = 512
STEPS = 2
SWEEPS = 2
R = 768
SUBS = 16
NROWS = 12288
POLES = 8


def make_orders(key):
    key_list = jax.random.split(jax.random.fold_in(key, 101), SUBS)
    return jax.vmap(lambda sub_key: jax.random.permutation(sub_key, ORDER))(key_list).astype(jnp.int32)


def draw_order_list(key, part):
    return make_orders(key)


def draw_inverse(key, part):
    orders = make_orders(key)
    places = jnp.argsort(orders, axis=1, stable=True).astype(jnp.int32)
    row_ids = jnp.arange(NROWS, dtype=jnp.int32)
    owner = row_ids // R
    local_row = row_ids % R
    column = places[owner, local_row + H]
    first_key, second_key, third_key = jax.random.split(jax.random.fold_in(key, 202), 3)
    columns = jnp.arange(2 * ORDER, dtype=jnp.int32)
    real_mark = (columns[None, :] == column[:, None]).astype(jnp.float32)
    imag_mark = (columns[None, :] == column[:, None] + ORDER).astype(jnp.float32)
    diag_re = 0.2 * jax.random.uniform(first_key, (POLES, NROWS, 1), jnp.float32, 0.6, 1.4)
    diag_im = 0.05 * jax.random.uniform(second_key, (POLES, NROWS, 1), jnp.float32, -1.0, 1.0)
    spread = 0.05 / ORDER ** 0.5
    jitter = spread * jax.random.normal(third_key, (POLES, NROWS, 2 * ORDER), jnp.float32)
    drawn = jitter + diag_re * real_mark[None] + diag_im * imag_mark[None]
    return drawn.astype(jnp.bfloat16)


def steps_of(rng, dims, shards, low, top_value):
    gain = 1.0
    for axis_at, blocks in shards:
        draws = jax.random.uniform(jax.random.fold_in(jax.random.fold_in(rng, 6), axis_at), (blocks,), jnp.float32, low / len(shards), top_value / len(shards))
        gain = gain * jnp.repeat(jnp.exp(draws), dims[axis_at] // blocks).reshape((-1,) + (1,) * (len(dims) - 1 - axis_at))
    return gain


def gaussian(key, shape, scale, bound, cuts=(), kind=jnp.bfloat16):
    loudness = steps_of(key, shape, cuts, -0.22, 0.18) if cuts else 1.0
    values = jax.random.normal(key, shape, jnp.float32) * scale * loudness
    return jnp.minimum(jnp.maximum(values, -bound), bound).astype(kind)


def setup_inputs(seed: int = 0) -> dict:
    streams_of = jax.random.split(jax.random.key(seed), 7)
    return {
        "state": gaussian(streams_of[0], (NROWS, SRC), 1.0, 6.0, ((0, 16),), jnp.float32),
        "conductivity": jnp.clip(jnp.exp(math.log(2.0) - 2.3025851 * jax.random.uniform(streams_of[1], (NROWS,), jnp.float32) ** steps_of(streams_of[1], (NROWS,), ((0, 16),), -0.2, 0.2)), 0.2, 2.0),
        "pole_shift": jnp.clip(0.2 + 0.8 * jax.random.uniform(streams_of[2], (POLES, 2), jnp.float32) ** steps_of(streams_of[2], (POLES, 2), ((0, 8),), -0.2, 0.2), 0.2, 1.0),
        "pole_weight": jnp.clip(jax.random.uniform(streams_of[3], (POLES, 2), jnp.float32, -1.5, 1.5) * steps_of(streams_of[3], (POLES, 2), ((0, 8),), -0.4, 0.0), -1.5, 1.5),
        "order_list": draw_order_list(jax.random.fold_in(streams_of[6], 71), 0),
        "inverse": draw_inverse(jax.random.fold_in(streams_of[6], 71), 0),
    }


def laplace(padded, rim_width):
    inner_count = padded.shape[0] - 2 * rim_width
    middle = padded[rim_width:rim_width + inner_count]
    return (4.0 * middle - padded[rim_width - 1:rim_width - 1 + inner_count]
            - padded[rim_width + 1:rim_width + 1 + inner_count]
            - padded[:inner_count] - padded[2 * rim_width:2 * rim_width + inner_count])


def shifted(padded, sigma_mid, shift_re, shift_im, rim_width):
    laplace_part = laplace(padded, rim_width)
    inner_count = laplace_part.shape[0]
    middle = padded[rim_width:rim_width + inner_count]
    column_half = middle.shape[1] // 2
    real_part = middle[:, :column_half]
    imag_part = middle[:, column_half:]
    sigma_col = sigma_mid[:, None]
    return laplace_part + jnp.concatenate(
        [sigma_col * (shift_re * real_part - shift_im * imag_part),
         sigma_col * (shift_im * real_part + shift_re * imag_part)], axis=1)


def correct(residual_ext, ordering, inverse_block):
    permuted = jnp.take(residual_ext, ordering.astype(jnp.int32), axis=0)
    column_half = permuted.shape[1] // 2
    real_part = permuted[:, :column_half]
    imag_part = permuted[:, column_half:]
    stacked = jnp.concatenate([jnp.concatenate([real_part, imag_part], axis=1),
                               jnp.concatenate([-imag_part, real_part], axis=1)], axis=0)
    return jnp.dot(inverse_block, stacked, preferred_element_type=jnp.float32)


def correct_all(residual, orderings, inverse_pole):
    padded = jnp.pad(residual, ((H, H), (0, 0)))

    def one_block(sub_index):
        extended = lax.dynamic_slice_in_dim(padded, sub_index * R, ORDER, 0)
        ordering = lax.dynamic_index_in_dim(orderings, sub_index, 0, keepdims=False)
        block = lax.dynamic_slice_in_dim(inverse_pole, sub_index * R, R, 0)
        return correct(extended, ordering, block)

    pieces = lax.map(one_block, jnp.arange(SUBS, dtype=jnp.int32))
    return pieces.reshape(NROWS, 2 * SRC)


def reference(state, conductivity, pole_shift, pole_weight, order_list, inverse):
    current = state
    for time_step in range(STEPS):
        right_side = conductivity[:, None] * current
        source = jnp.concatenate([right_side, jnp.zeros_like(right_side)], axis=1)
        summed = jnp.zeros_like(current)
        for pole_index in range(POLES):
            shift_re = pole_shift[pole_index, 0]
            shift_im = pole_shift[pole_index, 1]
            iterate = correct_all(source.astype(jnp.bfloat16), order_list, inverse[pole_index])
            for sweep_index in range(1, SWEEPS):
                padded = jnp.pad(iterate, ((H, H), (0, 0)))
                applied = shifted(padded, conductivity, shift_re, shift_im, H)
                residual = (source - applied).astype(jnp.bfloat16)
                iterate = iterate + correct_all(residual, order_list, inverse[pole_index])
            summed = summed + 2.0 * (pole_weight[pole_index, 0] * iterate[:, :SRC]
                                     - pole_weight[pole_index, 1] * iterate[:, SRC:])
        current = summed
    return current
```

```python
import jax
import jax.numpy as jnp
from jax import lax
from jax.experimental import pallas as pl
from jax.experimental.pallas import tpu as pltpu
from jax.sharding import PartitionSpec as P

MESH = pl.DeviceIdType.MESH
F32 = jnp.float32
BF16 = jnp.bfloat16
H = 128
N = 128
PEERS = ((2, 1), (1, 1), (3, 1), (2, 0), (0, 1), (1, 0), (3, 0))
EVERY = PEERS + ((0, 0),)
I16 = jnp.int16
TOP = 32767.0


def rounded(x):
    return x.astype(BF16)


def coded(v, peak):
    return jnp.round(v * (TOP / peak)).astype(jnp.int32).astype(I16)


def peak_of(v):
    return jnp.maximum(jnp.max(jnp.abs(v), axis=0, keepdims=True), 1e-30)


def decoded(q, peak):
    return q.astype(jnp.int32).astype(F32) * (peak * (1.0 / TOP))


def kernel(
    chunks, order_ref, cond_ref, shift_ref, weight_ref, state_hbm, inv_hbm, out_ref,
    g_in, st, cb, gp, e1, hs, x, acc, rp, p1s, p1r, p1sp, p1rp, e2, rss, rsr, rssp, rsrp,
    ags, agr, agsp, agrp, nbs,
    in_sem, halo_ss, halo_rs, p1_ss, p1_rs, rs_ss, rs_rs, ag_ss, ag_rs, nb_ss, nb_rs,
):
    s = lax.axis_index("sub")
    p = lax.axis_index("pole")
    px, pz = p // 2, lax.rem(p, 2)
    subs = lax.axis_size("sub")
    has_up, has_down = s > 0, s < subs - 1
    up, down = lax.rem(s + subs - 1, subs), lax.rem(s + 1, subs)

    def pole_at(dx, dz):
        return lax.rem(px + dx, 4) * 2 + lax.rem(pz + dz, 2)

    def remote(src, dst, send_sem, recv_sem, sub, pole):
        return pltpu.make_async_remote_copy(
            src_ref=src, dst_ref=dst, send_sem=send_sem, recv_sem=recv_sem,
            device_id=(sub, pole), device_id_type=MESH,
        )

    state_in = [
        pltpu.make_async_copy(state_hbm.at[:, pl.ds(c * N, N)], st.at[c], in_sem.at[c])
        for c in range(chunks)
    ]
    for copy in state_in:
        copy.start()
    g_copy = pltpu.make_async_copy(inv_hbm.at[0], g_in, in_sem.at[chunks])
    g_copy.start()

    barrier = pltpu.get_barrier_semaphore()
    for dx, dz in EVERY:
        q = pole_at(dx, dz)
        if (dx, dz) != (0, 0):
            pl.semaphore_signal(barrier, inc=1, device_id=(s, q), device_id_type=MESH)
        pl.semaphore_signal(barrier, inc=1, device_id=(up, q), device_id_type=MESH)
        pl.semaphore_signal(barrier, inc=1, device_id=(down, q), device_id_type=MESH)

    shift_re, shift_im = shift_ref[0, 0], shift_ref[0, 1]
    w_re, w_im = 2.0 * weight_ref[0, 0], 2.0 * weight_ref[0, 1]

    for b in range(6):
        row = cond_ref[:, 128 * b : 128 * b + 128]
        cb[128 * b : 128 * b + 128, :] = jnp.broadcast_to(row, (128, 128)).T

    for c in range(chunks):
        for d in range(2):
            x[c, d, 0:8, :] = jnp.zeros((8, N), F32)
            x[c, d, 776:784, :] = jnp.zeros((8, N), F32)

    @pl.when(jnp.logical_not(has_up))
    def _():
        for t in range(2):
            for c in range(chunks):
                e1[t, c, 768:896, :] = jnp.zeros((H, N), BF16)
                p1r[t, c, 0] = jnp.zeros((4, H, N), I16)
                p1rp[t, c, 0] = jnp.zeros((4, N), F32)

    @pl.when(jnp.logical_not(has_down))
    def _():
        for t in range(2):
            for c in range(chunks):
                e1[t, c, 896:1024, :] = jnp.zeros((H, N), BF16)
                p1r[t, c, 1] = jnp.zeros((4, H, N), I16)
                p1rp[t, c, 1] = jnp.zeros((4, N), F32)

    for copy in state_in:
        copy.wait()

    def first_source(c, _):
        src = cb[...] * st[c]
        st[c] = src
        e1[0, c, 0:512, :] = rounded(src[128:640])
        top = rounded(src[0:128])
        bottom = rounded(src[640:768])
        hs[c, 0] = top
        hs[c, 1] = bottom
        for q in range(8):
            e1[0, c, 512 + 32 * q : 528 + 32 * q, :] = top[16 * q : 16 * q + 16]
            e1[0, c, 528 + 32 * q : 544 + 32 * q, :] = bottom[16 * q : 16 * q + 16]
        return 0

    lax.fori_loop(0, chunks, first_source, 0)
    pl.semaphore_wait(barrier, 23)

    def halo_copy(c, d):
        return remote(
            hs.at[c, d], e1.at[0, c, pl.ds(896 - 128 * d, H)], halo_ss.at[c, d], halo_rs.at[c, d],
            down if d else up, p,
        )

    class Several:
        def __init__(self, *copies):
            self.copies = copies

        def start(self):
            for copy in self.copies:
                copy.start()

        def wait_recv(self):
            for copy in self.copies:
                copy.wait_recv()

        def wait_send(self):
            for copy in self.copies:
                copy.wait_send()

    def edge_copy(t, c, d):
        to = down if d else up
        return Several(
            remote(p1sp.at[t, c, d], p1rp.at[t, c, 1 - d], p1_ss.at[t, c, d, 1], p1_rs.at[t, c, d, 1], to, p),
            remote(p1s.at[t, c, d], p1r.at[t, c, 1 - d], p1_ss.at[t, c, d, 0], p1_rs.at[t, c, d, 0], to, p),
        )

    def start_both(make, *args):
        @pl.when(has_up)
        def _():
            make(*args, 0).start()

        @pl.when(has_down)
        def _():
            make(*args, 1).start()

    def wait_recv_both(make, *args):
        @pl.when(has_up)
        def _():
            make(*args, 1).wait_recv()

        @pl.when(has_down)
        def _():
            make(*args, 0).wait_recv()

    def wait_send_both(make, *args):
        @pl.when(has_up)
        def _():
            make(*args, 0).wait_send()

        @pl.when(has_down)
        def _():
            make(*args, 1).wait_send()

    def start_halo(c, _):
        start_both(halo_copy, c)
        return 0

    lax.fori_loop(0, chunks, start_halo, 0)

    g_copy.wait()

    def extended_row(base, count):
        return lax.broadcasted_iota(jnp.int32, (count, 1), 0) + base

    for blk in range(4):
        if blk < 2:
            rows = extended_row(256 + 256 * blk, 256)
        elif blk == 2:
            rows = jnp.concatenate(
                [extended_row(b + 16 * q, 16) for q in range(8) for b in (128, 768)], axis=0
            )
        else:
            rows = jnp.concatenate([extended_row(0, 128), extended_row(896, 128)], axis=0)
        hot = jnp.where(rows == order_ref[...], 1.0, 0.0).astype(BF16)
        at = 256 * blk
        for m in range(2):
            r0 = 384 * m
            re = lax.dot_general(
                g_in[r0 : r0 + 384, 0:1024], hot, (((1,), (1,)), ((), ())), preferred_element_type=F32
            )
            im = lax.dot_general(
                g_in[r0 : r0 + 384, 1024:2048], hot, (((1,), (1,)), ((), ())), preferred_element_type=F32
            )
            gp[r0 : r0 + 384, at : at + 256] = rounded(re)
            gp[768 + r0 : 768 + r0 + 384, at : at + 256] = rounded(im)

    def sweep_one(t, c):
        y = jnp.dot(gp[...], e1[t, c], preferred_element_type=F32)
        x[c, 0, 8:776, :] = y[:768]
        x[c, 1, 8:776, :] = y[768:]

    def residual(t, c):
        for b in (0, 5, 1, 2, 3, 4):
            at = 8 + 128 * b

            def lap(d):
                v = (
                    4.0 * x[c, d, at : at + 128, :]
                    - x[c, d, at - 1 : at + 127, :]
                    - x[c, d, at + 1 : at + 129, :]
                )
                if b > 0:
                    v = v - x[c, d, at - 128 : at, :]
                if b < 5:
                    v = v - x[c, d, at + 128 : at + 256, :]
                return v

            xr = x[c, 0, at : at + 128, :]
            xi = x[c, 1, at : at + 128, :]
            sigma = cb[128 * b : 128 * b + 128, :]
            src = st[c, 128 * b : 128 * b + 128, :]
            rr = src - lap(0) - sigma * (shift_re * xr - shift_im * xi)
            ri = -lap(1) - sigma * (shift_im * xr + shift_re * xi)
            acc[c, 128 * b : 128 * b + 128, :] = w_re * xr - w_im * xi
            if 0 < b < 5:
                e2[c, 128 * (b - 1) : 128 * b, 0:N] = rounded(rr)
                e2[c, 128 * (b - 1) : 128 * b, N : 2 * N] = rounded(ri)
            else:
                d = 0 if b == 0 else 1
                rp[c, d, 0] = rr
                rp[c, d, 1] = ri
                for i, v in enumerate((xr, xi, rr, ri)):
                    peak = peak_of(v)
                    p1sp[t, c, d, i : i + 1, :] = peak
                    p1s[t, c, d, i] = coded(v, peak)
        start_both(edge_copy, t, c)

    def weighted(y):
        re = y[:768, 0:N] - y[768:, N : 2 * N]
        im = y[:768, N : 2 * N] + y[768:, 0:N]
        return w_re * re - w_im * im

    def inner_product(c, _):
        acc[c] += weighted(jnp.dot(gp[:, 0:512], e2[c, 0:512, :], preferred_element_type=F32))
        return 0

    row_of = lax.broadcasted_iota(jnp.int32, (H, 1), 0)
    up_on = jnp.where(has_up, 1.0, 0.0).astype(F32)
    down_on = jnp.where(has_down, 1.0, 0.0).astype(F32)

    def rs_copy(t, c, k):
        q = pole_at(*PEERS[k])
        return Several(
            remote(rssp.at[t, c], rsrp.at[t, c, k], rs_ss.at[t, c, k, 1], rs_rs.at[t, c, k, 1], s, q),
            remote(rss.at[t, c, q], rsr.at[t, c, k], rs_ss.at[t, c, k, 0], rs_rs.at[t, c, k, 0], s, q),
        )

    def finish(t, c):
        wait_recv_both(edge_copy, t, c)
        for d in range(2):
            base = 512
            to = slice(N * d, N * d + N)

            def came(side, i):
                return decoded(p1r[t, c, side, i], p1rp[t, c, side, i : i + 1, :])

            above, below = came(0, d), came(1, d)
            top = rp[c, 0, d] + above + jnp.where(row_of == 0, above[127:128], 0.0)
            bottom = rp[c, 1, d] + below + jnp.where(row_of == 127, below[0:1], 0.0)
            top, bottom = rounded(top), rounded(bottom)
            for q in range(8):
                e2[c, base + 32 * q : base + 32 * q + 16, to] = top[16 * q : 16 * q + 16]
                e2[c, base + 32 * q + 16 : base + 32 * q + 32, to] = bottom[16 * q : 16 * q + 16]
            first = x[c, d, 8:136, :]
            final = x[c, d, 648:776, :]
            over = came(0, 2 + d) + first + jnp.where(row_of == 127, first[0:1], 0.0)
            under = came(1, 2 + d) + final + jnp.where(row_of == 0, final[127:128], 0.0)
            e2[c, base + 256 : base + 384, to] = rounded(up_on * over)
            e2[c, base + 384 : base + 512, to] = rounded(down_on * under)
        total = acc[c] + weighted(jnp.dot(gp[:, 512:1024], e2[c, 512:1024, :], preferred_element_type=F32))
        peak = peak_of(total)
        rssp[t, c] = peak
        total = coded(total, peak)
        for q in range(8):
            if t == 0:
                rss[t, c, q, 0:64, :] = total[128 + 64 * q : 192 + 64 * q]
                rss[t, c, q, 64:80, :] = total[16 * q : 16 * q + 16]
                rss[t, c, q, 80:96, :] = total[640 + 16 * q : 656 + 16 * q]
            else:
                rss[t, c, q] = total[96 * q : 96 * q + 96]
        for k in range(7):
            rs_copy(t, c, k).start()

    def summed(t, c):
        total = decoded(rss[t, c, p], rssp[t, c])
        for k in range(7):
            rs_copy(t, c, k).wait_recv()
        for k in range(7):
            total = total + decoded(rsr[t, c, k], rsrp[t, c, k])
        return total

    def ag_copy(c, k):
        q = pole_at(*PEERS[k])
        return Several(
            remote(agsp.at[c], agrp.at[c, k], ag_ss.at[c, k, 1], ag_rs.at[c, k, 1], s, q),
            remote(ags.at[c], agr.at[c, k], ag_ss.at[c, k, 0], ag_rs.at[c, k, 0], s, q),
        )

    def margin_copy(c, k, d):
        q = pole_at(*EVERY[k])
        src = nbs.at[c, d]
        dst = e1.at[1, c, pl.ds(pl.multiple_of(896 - 128 * d + 16 * p, 16), 16)]
        return remote(src, dst, nb_ss.at[c, k, d], nb_rs.at[c, k, d], down if d else up, q)

    def placed_share(c, q, share):
        st[c, pl.ds(pl.multiple_of(128 + 64 * q, 64), 64), :] = share[0:64]
        st[c, pl.ds(pl.multiple_of(16 * q, 16), 16), :] = share[64:80]
        st[c, pl.ds(pl.multiple_of(640 + 16 * q, 16), 16), :] = share[80:96]
        share = rounded(share)
        e1[1, c, pl.ds(pl.multiple_of(64 * q, 64), 64), :] = share[0:64]
        e1[1, c, pl.ds(pl.multiple_of(512 + 32 * q, 32), 32), :] = share[64:96]

    def next_source(c, _):
        total = summed(0, c)
        sigma = jnp.concatenate(
            [
                cb[pl.ds(pl.multiple_of(128 + 64 * p, 64), 64), :],
                cb[pl.ds(pl.multiple_of(16 * p, 16), 16), :],
                cb[pl.ds(pl.multiple_of(640 + 16 * p, 16), 16), :],
            ],
            axis=0,
        )
        share = sigma * total
        peak = peak_of(share)
        agsp[c] = peak
        ags[c] = coded(share, peak)
        edges = rounded(share[64:96])
        nbs[c, 0] = edges[0:16]
        nbs[c, 1] = edges[16:32]
        for k in range(7):
            ag_copy(c, k).start()

        @pl.when(has_up)
        def _():
            for k in range(8):
                margin_copy(c, k, 0).start()

        @pl.when(has_down)
        def _():
            for k in range(8):
                margin_copy(c, k, 1).start()

        placed_share(c, p, share)
        return 0

    def source_arrived(c):
        for k, (dx, dz) in enumerate(PEERS):
            ag_copy(c, k).wait_recv()
            placed_share(c, pole_at(4 - dx, dz), decoded(agr[c, k], agrp[c, k]))

        @pl.when(has_up)
        def _():
            for k in range(8):
                margin_copy(c, k, 1).wait_recv()

        @pl.when(has_down)
        def _():
            for k in range(8):
                margin_copy(c, k, 0).wait_recv()

    def first_sweep(c, _):
        wait_recv_both(halo_copy, c)
        sweep_one(0, c)
        residual(0, c)
        return 0

    lax.fori_loop(0, chunks, first_sweep, 0)
    lax.fori_loop(0, chunks, inner_product, 0)

    def second_sweep(c, _):
        finish(0, c)
        return 0

    lax.fori_loop(0, chunks, second_sweep, 0)
    lax.fori_loop(0, chunks, next_source, 0)

    def first_sweep_again(c, _):
        source_arrived(c)
        sweep_one(1, c)
        residual(1, c)
        inner_product(c, 0)
        return 0

    lax.fori_loop(0, chunks, first_sweep_again, 0)

    def second_sweep_again(c, _):
        finish(1, c)
        return 0

    lax.fori_loop(0, chunks, second_sweep_again, 0)
    for c in range(chunks):
        out_ref[:, c * N : c * N + N] = summed(1, c)

    def drain(c, _):
        wait_send_both(halo_copy, c)
        for t in range(2):
            wait_send_both(edge_copy, t, c)
            for k in range(7):
                rs_copy(t, c, k).wait_send()
        for k in range(7):
            ag_copy(c, k).wait_send()

        @pl.when(has_up)
        def _():
            for k in range(8):
                margin_copy(c, k, 0).wait_send()

        @pl.when(has_down)
        def _():
            for k in range(8):
                margin_copy(c, k, 1).wait_send()

        return 0

    lax.fori_loop(0, chunks, drain, 0)


def shards(state, conductivity, pole_shift, pole_weight, order_list, inverse):
    rows, columns = state.shape
    chunks = columns // N
    vmem = pl.BlockSpec(memory_space=pltpu.VMEM)
    smem = pl.BlockSpec(memory_space=pltpu.SMEM)
    anywhere = pl.BlockSpec(memory_space=pl.ANY)
    dma = pltpu.SemaphoreType.DMA

    def body(*refs):
        kernel(chunks, *refs)

    return pl.pallas_call(
        body,
        out_shape=jax.ShapeDtypeStruct((rows // 8, columns), F32),
        in_specs=[vmem, vmem, smem, smem, anywhere, anywhere],
        out_specs=vmem,
        scratch_shapes=[
            pltpu.VMEM((768, 2048), BF16),
            pltpu.VMEM((chunks, 768, N), F32),
            pltpu.VMEM((768, N), F32),
            pltpu.VMEM((1536, 1024), BF16),
            pltpu.VMEM((2, chunks, 1024, N), BF16),
            pltpu.VMEM((chunks, 2, H, N), BF16),
            pltpu.VMEM((chunks, 2, 784, N), F32),
            pltpu.VMEM((chunks, 768, N), F32),
            pltpu.VMEM((chunks, 2, 2, H, N), F32),
            pltpu.VMEM((2, chunks, 2, 4, H, N), I16),
            pltpu.VMEM((2, chunks, 2, 4, H, N), I16),
            pltpu.VMEM((2, chunks, 2, 4, N), F32),
            pltpu.VMEM((2, chunks, 2, 4, N), F32),
            pltpu.VMEM((chunks, 1024, 2 * N), BF16),
            pltpu.VMEM((2, chunks, 8, 96, N), I16),
            pltpu.VMEM((2, chunks, 7, 96, N), I16),
            pltpu.VMEM((2, chunks, 1, N), F32),
            pltpu.VMEM((2, chunks, 7, 1, N), F32),
            pltpu.VMEM((chunks, 96, N), I16),
            pltpu.VMEM((chunks, 7, 96, N), I16),
            pltpu.VMEM((chunks, 1, N), F32),
            pltpu.VMEM((chunks, 7, 1, N), F32),
            pltpu.VMEM((chunks, 2, 16, N), BF16),
            dma((chunks + 1,)),
            dma((chunks, 2)),
            dma((chunks, 2)),
            dma((2, chunks, 2, 2)),
            dma((2, chunks, 2, 2)),
            dma((2, chunks, 7, 2)),
            dma((2, chunks, 7, 2)),
            dma((chunks, 7, 2)),
            dma((chunks, 7, 2)),
            dma((chunks, 8, 2)),
            dma((chunks, 8, 2)),
        ],
        compiler_params=pltpu.CompilerParams(
            collective_id=0, has_side_effects=True, vmem_limit_bytes=58 << 20
        ),
    )(order_list, conductivity.reshape(1, rows), pole_shift, pole_weight, state, inverse)


def solution(mesh):
    placed = (
        P("sub", None),
        P("sub"),
        P("pole", None),
        P("pole", None),
        P("sub", None),
        P("pole", "sub", None),
    )
    return jax.shard_map(
        shards, mesh=mesh, in_specs=placed, out_specs=P(("sub", "pole"), None), check_vma=False
    )
```

```python
import jax
import jax.numpy as jnp
from jax import lax
from jax.experimental import pallas as pl
from jax.experimental.pallas import tpu as pltpu
from jax.sharding import PartitionSpec as P

MESH = pl.DeviceIdType.MESH
F32 = jnp.float32
BF16 = jnp.bfloat16
H = 128
N = 128
PAIR = 2 * N
PEERS = ((2, 1), (1, 1), (3, 1), (2, 0), (0, 1), (1, 0), (3, 0))
I16 = jnp.int16
TOP = 32767.0


def rounded(x):
    return x.astype(BF16)


def coded(v, peak):
    return jnp.round(v * (TOP / peak)).astype(jnp.int32).astype(I16)


def peak_of(v):
    return jnp.maximum(jnp.max(jnp.abs(v), axis=0, keepdims=True), 1e-30)


def decoded(q, peak):
    return q.astype(jnp.int32).astype(F32) * (peak * (1.0 / TOP))


def kernel(
    chunks, order_ref, cond_ref, shift_ref, weight_ref, state_hbm, inv_hbm, out_ref,
    g_in, st, cb, gp, e1, hs, x, acc, rp, p1s, p1r, p1sp, p1rp, e2, rss, rsr, rssp, rsrp,
    ags, agr, agsp, agrp, res,
    in_sem, halo_ss, halo_rs, p1_ss, p1_rs, rs_ss, rs_rs, ag_ss, ag_rs,
):
    pairs = chunks // 2
    s = lax.axis_index("sub")
    p = lax.axis_index("pole")
    px, pz = p // 2, lax.rem(p, 2)
    subs = lax.axis_size("sub")
    has_up, has_down = s > 0, s < subs - 1
    up, down = lax.rem(s + subs - 1, subs), lax.rem(s + 1, subs)

    def pole_at(dx, dz):
        return lax.rem(px + dx, 4) * 2 + lax.rem(pz + dz, 2)

    def remote(src, dst, send_sem, recv_sem, sub, pole):
        return pltpu.make_async_remote_copy(
            src_ref=src, dst_ref=dst, send_sem=send_sem, recv_sem=recv_sem,
            device_id=(sub, pole), device_id_type=MESH,
        )

    state_in = [
        pltpu.make_async_copy(state_hbm.at[:, pl.ds(c * N, N)], st.at[c], in_sem.at[0])
        for c in range(chunks)
    ]
    for copy in state_in:
        copy.start()
    g_copy = pltpu.make_async_copy(inv_hbm.at[0], g_in, in_sem.at[1])
    g_copy.start()

    barrier = pltpu.get_barrier_semaphore()
    for dx, dz in PEERS:
        pl.semaphore_signal(barrier, inc=1, device_id=(s, pole_at(dx, dz)), device_id_type=MESH)
    pl.semaphore_signal(barrier, inc=1, device_id=(up, p), device_id_type=MESH)
    pl.semaphore_signal(barrier, inc=1, device_id=(down, p), device_id_type=MESH)

    shift_re, shift_im = shift_ref[0, 0], shift_ref[0, 1]
    w_re, w_im = 2.0 * weight_ref[0, 0], 2.0 * weight_ref[0, 1]

    for b in range(6):
        row = cond_ref[128 * b : 128 * b + 128]
        cb[128 * b : 128 * b + 128, :] = jnp.broadcast_to(row[None, :], (128, 128)).T

    for c in range(chunks):
        for d in range(2):
            x[c, d, 0:8, :] = jnp.zeros((8, N), F32)
            x[c, d, 776:784, :] = jnp.zeros((8, N), F32)

    @pl.when(jnp.logical_not(has_up))
    def _():
        for t in range(2):
            for j in range(pairs):
                e1[t, j, 768:896, :] = jnp.zeros((H, PAIR), BF16)
            for c in range(chunks):
                p1r[0, t, c] = jnp.zeros((4, H, N), I16)
                p1rp[0, t, c] = jnp.zeros((4, N), F32)

    @pl.when(jnp.logical_not(has_down))
    def _():
        for t in range(2):
            for j in range(pairs):
                e1[t, j, 896:1024, :] = jnp.zeros((H, PAIR), BF16)
            for c in range(chunks):
                p1r[1, t, c] = jnp.zeros((4, H, N), I16)
                p1rp[1, t, c] = jnp.zeros((4, N), F32)

    pltpu.make_async_copy(st, st, in_sem.at[0]).wait()
    for c in range(chunks):
        j, to = c // 2, slice(N * (c % 2), N * (c % 2) + N)
        src = cb[...] * st[c]
        st[c] = src
        e1[0, j, 0:512, to] = rounded(src[128:640])
        top = rounded(src[0:128])
        bottom = rounded(src[640:768])
        hs[0, 0, j, :, to] = top
        hs[1, 0, j, :, to] = bottom
        for q in range(8):
            e1[0, j, 512 + 32 * q : 528 + 32 * q, to] = top[16 * q : 16 * q + 16]
            e1[0, j, 528 + 32 * q : 544 + 32 * q, to] = bottom[16 * q : 16 * q + 16]

    def halo_copy(t, j, d):
        return remote(
            hs.at[d, t, j], e1.at[t, j, pl.ds(896 - 128 * d, H)], halo_ss.at[d], halo_rs.at[t, j, d],
            down if d else up, p,
        )

    class Several:
        def __init__(self, *copies):
            self.copies = copies

        def start(self):
            for copy in self.copies:
                copy.start()

        def wait_recv(self):
            for copy in self.copies:
                copy.wait_recv()

        def wait_send(self):
            for copy in self.copies:
                copy.wait_send()

    def edge_copy(t, c, d):
        to = down if d else up
        return Several(
            remote(p1sp.at[d, t, c], p1rp.at[1 - d, t, c], p1_ss.at[d, 1], p1_rs.at[t, c, d, 1], to, p),
            remote(p1s.at[d, t, c], p1r.at[1 - d, t, c], p1_ss.at[d, 0], p1_rs.at[t, c, d, 0], to, p),
        )

    def start_both(make, *args):
        @pl.when(has_up)
        def _():
            make(*args, 0).start()

        @pl.when(has_down)
        def _():
            make(*args, 1).start()

    def wait_recv_both(make, *args):
        @pl.when(has_up)
        def _():
            make(*args, 1).wait_recv()

        @pl.when(has_down)
        def _():
            make(*args, 0).wait_recv()

    g_copy.wait()
    order = order_ref[...]

    def extended_row(base, count):
        return lax.broadcasted_iota(jnp.int32, (count, 1), 0) + base

    for blk in range(4):
        if blk == 2:
            pl.semaphore_wait(barrier, 9)
            for j in range(pairs):
                start_both(halo_copy, 0, j)
        if blk < 2:
            rows = extended_row(256 + 256 * blk, 256)
        elif blk == 2:
            rows = jnp.concatenate(
                [extended_row(b + 16 * q, 16) for q in range(8) for b in (128, 768)], axis=0
            )
        else:
            rows = jnp.concatenate([extended_row(0, 128), extended_row(896, 128)], axis=0)
        hot = jnp.where(rows == order, 1.0, 0.0).astype(BF16)
        at = 256 * blk
        for m in range(2):
            r0 = 384 * m
            re = lax.dot_general(
                g_in[r0 : r0 + 384, 0:1024], hot, (((1,), (1,)), ((), ())), preferred_element_type=F32
            )
            im = lax.dot_general(
                g_in[r0 : r0 + 384, 1024:2048], hot, (((1,), (1,)), ((), ())), preferred_element_type=F32
            )
            gp[r0 : r0 + 384, at : at + 256] = rounded(re)
            gp[768 + r0 : 768 + r0 + 384, at : at + 256] = rounded(im)

    def own_sweep(t, j):
        y = jnp.dot(gp[:, 0:768], e1[t, j, 0:768, :], preferred_element_type=F32)
        for i in range(2):
            for d in range(2):
                x[2 * j + i, d, 8:776, :] = y[768 * d : 768 * d + 768, N * i : N * i + N]

    def margin_sweep(t, j):
        y = jnp.dot(gp[:, 768:1024], e1[t, j, 768:1024, :], preferred_element_type=F32)
        for i in range(2):
            for d in range(2):
                x[2 * j + i, d, 8:776, :] += y[768 * d : 768 * d + 768, N * i : N * i + N]

    def residual(t, c):
        for b in (0, 5, 1, 2, 3, 4):
            at = 8 + 128 * b

            def lap(d):
                v = (
                    4.0 * x[c, d, at : at + 128, :]
                    - x[c, d, at - 1 : at + 127, :]
                    - x[c, d, at + 1 : at + 129, :]
                )
                if b > 0:
                    v = v - x[c, d, at - 128 : at, :]
                if b < 5:
                    v = v - x[c, d, at + 128 : at + 256, :]
                return v

            xr = x[c, 0, at : at + 128, :]
            xi = x[c, 1, at : at + 128, :]
            sigma = cb[128 * b : 128 * b + 128, :]
            src = st[c, 128 * b : 128 * b + 128, :]
            rr = src - lap(0) - sigma * (shift_re * xr - shift_im * xi)
            ri = -lap(1) - sigma * (shift_im * xr + shift_re * xi)
            acc[c, 128 * b : 128 * b + 128, :] = w_re * xr - w_im * xi
            if 0 < b < 5:
                e2[c, 128 * (b - 1) : 128 * b, 0:N] = rounded(rr)
                e2[c, 128 * (b - 1) : 128 * b, N : 2 * N] = rounded(ri)
            else:
                d = 0 if b == 0 else 1
                rp[c, d, 0] = rr
                rp[c, d, 1] = ri
                for i, v in enumerate((xr, xi, rr, ri)):
                    peak = peak_of(v)
                    p1sp[d, t, c, i : i + 1, :] = peak
                    p1s[d, t, c, i] = coded(v, peak)
        start_both(edge_copy, t, c)

    def weighted(y):
        re = y[:768, 0:N] - y[768:, N : 2 * N]
        im = y[:768, N : 2 * N] + y[768:, 0:N]
        return w_re * re - w_im * im

    def inner_product(c, _):
        acc[c] += weighted(jnp.dot(gp[:, 0:512], e2[c, 0:512, :], preferred_element_type=F32))
        return 0

    row_of = lax.broadcasted_iota(jnp.int32, (H, 1), 0)
    up_on = jnp.where(has_up, 1.0, 0.0).astype(F32)
    down_on = jnp.where(has_down, 1.0, 0.0).astype(F32)

    def rs_copy(t, c, k):
        q = pole_at(*PEERS[k])
        return Several(
            remote(rssp.at[t, c], rsrp.at[t, c, k], rs_ss.at[1], rs_rs.at[t, c, 1], s, q),
            remote(rss.at[t, c, q], rsr.at[t, c, k], rs_ss.at[0], rs_rs.at[t, c, 0], s, q),
        )

    def finish(t, c):
        wait_recv_both(edge_copy, t, c)
        for d in range(2):
            base = 512
            to = slice(N * d, N * d + N)

            def came(side, i):
                return decoded(p1r[side, t, c, i], p1rp[side, t, c, i : i + 1, :])

            above, below = came(0, d), came(1, d)
            top = rp[c, 0, d] + above + jnp.where(row_of == 0, above[127:128], 0.0)
            bottom = rp[c, 1, d] + below + jnp.where(row_of == 127, below[0:1], 0.0)
            top, bottom = rounded(top), rounded(bottom)
            for q in range(8):
                e2[c, base + 32 * q : base + 32 * q + 16, to] = top[16 * q : 16 * q + 16]
                e2[c, base + 32 * q + 16 : base + 32 * q + 32, to] = bottom[16 * q : 16 * q + 16]
            first = x[c, d, 8:136, :]
            final = x[c, d, 648:776, :]
            over = came(0, 2 + d) + first + jnp.where(row_of == 127, first[0:1], 0.0)
            under = came(1, 2 + d) + final + jnp.where(row_of == 0, final[127:128], 0.0)
            e2[c, base + 256 : base + 384, to] = rounded(up_on * over)
            e2[c, base + 384 : base + 512, to] = rounded(down_on * under)
        total = acc[c] + weighted(jnp.dot(gp[:, 512:1024], e2[c, 512:1024, :], preferred_element_type=F32))
        peak = peak_of(total)
        rssp[t, c] = peak
        total = coded(total, peak)
        for q in range(8):
            if t == 0:
                rss[t, c, q, 0:64, :] = total[128 + 64 * q : 192 + 64 * q]
                rss[t, c, q, 64:80, :] = total[16 * q : 16 * q + 16]
                rss[t, c, q, 80:96, :] = total[640 + 16 * q : 656 + 16 * q]
            else:
                rss[t, c, q] = total[96 * q : 96 * q + 96]
        for k in range(7):
            rs_copy(t, c, k).start()

    def all_came(ref, sem):
        pltpu.make_async_copy(ref, ref, sem).wait()

    def summed(t, c):
        total = decoded(rss[t, c, p], rssp[t, c])
        all_came(rsrp.at[t, c], rs_rs.at[t, c, 1])
        all_came(rsr.at[t, c], rs_rs.at[t, c, 0])
        for k in range(7):
            total = total + decoded(rsr[t, c, k], rsrp[t, c, k])
        return total

    def ag_copy(c, k):
        q = pole_at(*PEERS[k])
        return Several(
            remote(agsp.at[c], agrp.at[c, k], ag_ss.at[1], ag_rs.at[c, 1], s, q),
            remote(ags.at[c], agr.at[c, k], ag_ss.at[0], ag_rs.at[c, 0], s, q),
        )

    def placed_share(j, i, q, share):
        c, to = 2 * j + i, slice(N * i, N * i + N)
        st[c, pl.ds(pl.multiple_of(128 + 64 * q, 64), 64), :] = share[0:64]
        st[c, pl.ds(pl.multiple_of(16 * q, 16), 16), :] = share[64:80]
        st[c, pl.ds(pl.multiple_of(640 + 16 * q, 16), 16), :] = share[80:96]
        share = rounded(share)
        e1[1, j, pl.ds(pl.multiple_of(64 * q, 64), 64), to] = share[0:64]
        e1[1, j, pl.ds(pl.multiple_of(512 + 32 * q, 32), 32), to] = share[64:96]
        hs[0, 1, j, pl.ds(pl.multiple_of(16 * q, 16), 16), to] = share[64:80]
        hs[1, 1, j, pl.ds(pl.multiple_of(16 * q, 16), 16), to] = share[80:96]

    def next_source(j, i):
        c = 2 * j + i
        total = summed(0, c)
        sigma = jnp.concatenate(
            [
                cb[pl.ds(pl.multiple_of(128 + 64 * p, 64), 64), :],
                cb[pl.ds(pl.multiple_of(16 * p, 16), 16), :],
                cb[pl.ds(pl.multiple_of(640 + 16 * p, 16), 16), :],
            ],
            axis=0,
        )
        share = sigma * total
        peak = peak_of(share)
        agsp[c] = peak
        ags[c] = coded(share, peak)
        for k in range(7):
            ag_copy(c, k).start()
        placed_share(j, i, p, share)

    def source_arrived(j):
        for i in range(2):
            c = 2 * j + i
            all_came(agrp.at[c], ag_rs.at[c, 1])
            all_came(agr.at[c], ag_rs.at[c, 0])
            for k, (dx, dz) in enumerate(PEERS):
                placed_share(j, i, pole_at(4 - dx, dz), decoded(agr[c, k], agrp[c, k]))
        start_both(halo_copy, 1, j)

    def over_pairs(step, *args):
        def body(j, _):
            step(*args, j)
            return 0

        lax.fori_loop(0, pairs, body, 0)

    def first_sweep(t, j):
        wait_recv_both(halo_copy, t, j)
        margin_sweep(t, j)

        def body(i, _):
            residual(t, 2 * j + i)
            return 0

        lax.fori_loop(0, 2, body, 0)

    def second_sweep(t):
        def body(c, _):
            finish(t, c)
            return 0

        lax.fori_loop(0, chunks, inner_product, 0)
        lax.fori_loop(0, chunks, body, 0)

    def both_next(j):
        for i in range(2):
            next_source(j, i)

    def source_in(j):
        source_arrived(j)
        own_sweep(1, j)

    over_pairs(own_sweep, 0)
    over_pairs(first_sweep, 0)
    second_sweep(0)
    over_pairs(both_next)
    over_pairs(source_in)
    over_pairs(first_sweep, 1)
    second_sweep(1)

    for c in range(chunks):
        res[:, c * N : c * N + N] = summed(1, c)
        pltpu.make_async_copy(
            res.at[:, pl.ds(c * N, N)], out_ref.at[:, pl.ds(c * N, N)], in_sem.at[0]
        ).start()

    all_came(rsr, rs_ss.at[0])
    all_came(rsrp, rs_ss.at[1])
    all_came(agr, ag_ss.at[0])
    all_came(agrp, ag_ss.at[1])

    def all_left(d):
        all_came(hs.at[d], halo_ss.at[d])
        all_came(p1s.at[d], p1_ss.at[d, 0])
        all_came(p1sp.at[d], p1_ss.at[d, 1])

    @pl.when(has_up)
    def _():
        all_left(0)

    @pl.when(has_down)
    def _():
        all_left(1)

    all_came(res, in_sem.at[0])


def shards(state, conductivity, pole_shift, pole_weight, order_list, inverse):
    rows, columns = state.shape
    chunks = columns // N
    vmem = pl.BlockSpec(memory_space=pltpu.VMEM)
    smem = pl.BlockSpec(memory_space=pltpu.SMEM)
    anywhere = pl.BlockSpec(memory_space=pl.ANY)
    dma = pltpu.SemaphoreType.DMA

    def body(*refs):
        kernel(chunks, *refs)

    return pl.pallas_call(
        body,
        out_shape=jax.ShapeDtypeStruct((rows // 8, columns), F32),
        in_specs=[vmem, vmem, smem, smem, anywhere, anywhere],
        out_specs=anywhere,
        scratch_shapes=[
            pltpu.VMEM((768, 2048), BF16),
            pltpu.VMEM((chunks, 768, N), F32),
            pltpu.VMEM((768, N), F32),
            pltpu.VMEM((1536, 1024), BF16),
            pltpu.VMEM((2, chunks // 2, 1024, PAIR), BF16),
            pltpu.VMEM((2, 2, chunks // 2, H, PAIR), BF16),
            pltpu.VMEM((chunks, 2, 784, N), F32),
            pltpu.VMEM((chunks, 768, N), F32),
            pltpu.VMEM((chunks, 2, 2, H, N), F32),
            pltpu.VMEM((2, 2, chunks, 4, H, N), I16),
            pltpu.VMEM((2, 2, chunks, 4, H, N), I16),
            pltpu.VMEM((2, 2, chunks, 4, N), F32),
            pltpu.VMEM((2, 2, chunks, 4, N), F32),
            pltpu.VMEM((chunks, 1024, 2 * N), BF16),
            pltpu.VMEM((2, chunks, 8, 96, N), I16),
            pltpu.VMEM((2, chunks, 7, 96, N), I16),
            pltpu.VMEM((2, chunks, 1, N), F32),
            pltpu.VMEM((2, chunks, 7, 1, N), F32),
            pltpu.VMEM((chunks, 96, N), I16),
            pltpu.VMEM((chunks, 7, 96, N), I16),
            pltpu.VMEM((chunks, 1, N), F32),
            pltpu.VMEM((chunks, 7, 1, N), F32),
            pltpu.VMEM((96, chunks * N), F32),
            dma((2,)),
            dma((2,)),
            dma((2, chunks // 2, 2)),
            dma((2, 2)),
            dma((2, chunks, 2, 2)),
            dma((2,)),
            dma((2, chunks, 2)),
            dma((2,)),
            dma((chunks, 2)),
        ],
        compiler_params=pltpu.CompilerParams(
            collective_id=0, has_side_effects=True, vmem_limit_bytes=58 << 20
        ),
    )(order_list, conductivity, pole_shift, pole_weight, state, inverse)


def solution(mesh):
    placed = (
        P("sub", None),
        P("sub"),
        P("pole", None),
        P("pole", None),
        P("sub", None),
        P("pole", "sub", None),
    )
    return jax.shard_map(
        shards, mesh=mesh, in_specs=placed, out_specs=P(("sub", "pole"), None), check_vma=False
    )
```

```python
import jax
import jax.numpy as jnp
from jax import lax
from jax.experimental import pallas as pl
from jax.experimental.pallas import tpu as pltpu
from jax.sharding import PartitionSpec as P

MESH = pl.DeviceIdType.MESH
F32 = jnp.float32
BF16 = jnp.bfloat16
H = 128
N = 128
PAIR = 2 * N
PEERS = ((2, 1), (1, 1), (3, 1), (2, 0), (0, 1), (1, 0), (3, 0))
EVERY = PEERS + ((0, 0),)
I16 = jnp.int16
TOP = 32767.0


def rounded(x):
    return x.astype(BF16)


def coded(v, peak):
    return jnp.round(v * (TOP / peak)).astype(jnp.int32).astype(I16)


def peak_of(v):
    return jnp.maximum(jnp.max(jnp.abs(v), axis=0, keepdims=True), 1e-30)


def decoded(q, peak):
    return q.astype(jnp.int32).astype(F32) * (peak * (1.0 / TOP))


def kernel(
    chunks, order_ref, cond_ref, shift_ref, weight_ref, state_hbm, inv_hbm, out_ref,
    g_in, st, cb, gp, e1, hs, x, acc, rp, p1s, p1r, p1sp, p1rp, e2, rss, rsr, rssp, rsrp,
    ags, agm, age, agsp, agrp, nbs, res,
    in_sem, halo_ss, halo_rs, p1_ss, p1_rs, rs_ss, rs_rs, ag_ss, ag_rs, nb_ss, nb_rs,
):
    pairs = chunks // 2
    s = lax.axis_index("sub")
    p = lax.axis_index("pole")
    px, pz = p // 2, lax.rem(p, 2)
    subs = lax.axis_size("sub")
    has_up, has_down = s > 0, s < subs - 1
    up, down = lax.rem(s + subs - 1, subs), lax.rem(s + 1, subs)

    def pole_at(dx, dz):
        return lax.rem(px + dx, 4) * 2 + lax.rem(pz + dz, 2)

    def remote(src, dst, send_sem, recv_sem, sub, pole):
        return pltpu.make_async_remote_copy(
            src_ref=src, dst_ref=dst, send_sem=send_sem, recv_sem=recv_sem,
            device_id=(sub, pole), device_id_type=MESH,
        )

    state_in = [
        pltpu.make_async_copy(state_hbm.at[:, pl.ds(c * N, N)], st.at[c], in_sem.at[0])
        for c in range(chunks)
    ]
    for copy in state_in:
        copy.start()
    for b in range(4):
        part = pl.ds(192 * b, 192)
        pltpu.make_async_copy(inv_hbm.at[0, part], g_in.at[part], in_sem.at[1]).start()

    barrier = pltpu.get_barrier_semaphore()
    for dx, dz in PEERS:
        pl.semaphore_signal(barrier, inc=1, device_id=(s, pole_at(dx, dz)), device_id_type=MESH)
    pl.semaphore_signal(barrier, inc=1, device_id=(up, p), device_id_type=MESH)
    pl.semaphore_signal(barrier, inc=1, device_id=(down, p), device_id_type=MESH)

    shift_re, shift_im = shift_ref[0, 0], shift_ref[0, 1]
    w_re, w_im = 2.0 * weight_ref[0, 0], 2.0 * weight_ref[0, 1]

    for b in range(6):
        row = cond_ref[128 * b : 128 * b + 128]
        cb[128 * b : 128 * b + 128, :] = jnp.broadcast_to(row[None, :], (128, 128)).T

    for c in range(chunks):
        for d in range(2):
            x[c, d, 0:8, :] = jnp.zeros((8, N), F32)
            x[c, d, 776:784, :] = jnp.zeros((8, N), F32)

    @pl.when(jnp.logical_not(has_up))
    def _():
        for t in range(2):
            for j in range(pairs):
                e1[t, j, 768:896, :] = jnp.zeros((H, PAIR), BF16)
            for c in range(chunks):
                p1r[0, t, c] = jnp.zeros((4, H, N), I16)
                p1rp[0, t, c] = jnp.zeros((4, N), F32)

    @pl.when(jnp.logical_not(has_down))
    def _():
        for t in range(2):
            for j in range(pairs):
                e1[t, j, 896:1024, :] = jnp.zeros((H, PAIR), BF16)
            for c in range(chunks):
                p1r[1, t, c] = jnp.zeros((4, H, N), I16)
                p1rp[1, t, c] = jnp.zeros((4, N), F32)

    pltpu.make_async_copy(st, st, in_sem.at[0]).wait()
    for c in range(chunks):
        j, to = c // 2, slice(N * (c % 2), N * (c % 2) + N)
        src = cb[...] * st[c]
        st[c] = src
        e1[0, j, 0:512, to] = rounded(src[128:640])
        top = rounded(src[0:128])
        bottom = rounded(src[640:768])
        hs[0, j, :, to] = top
        hs[1, j, :, to] = bottom
        for q in range(8):
            e1[0, j, 512 + 32 * q : 528 + 32 * q, to] = top[16 * q : 16 * q + 16]
            e1[0, j, 528 + 32 * q : 544 + 32 * q, to] = bottom[16 * q : 16 * q + 16]

    def halo_copy(t, j, d):
        return remote(
            hs.at[d, pairs * t + j], e1.at[t, j, pl.ds(896 - 128 * d, H)], halo_ss.at[d], halo_rs.at[t, j, d],
            down if d else up, p,
        )

    class Several:
        def __init__(self, *copies):
            self.copies = copies

        def start(self):
            for copy in self.copies:
                copy.start()

        def wait_recv(self):
            for copy in self.copies:
                copy.wait_recv()

        def wait_send(self):
            for copy in self.copies:
                copy.wait_send()

    def edge_copy(t, c, d):
        to = down if d else up
        return Several(
            remote(p1sp.at[d, t, c], p1rp.at[1 - d, t, c], p1_ss.at[d, 1], p1_rs.at[t, c, d, 1], to, p),
            remote(p1s.at[d, t, c], p1r.at[1 - d, t, c], p1_ss.at[d, 0], p1_rs.at[t, c, d, 0], to, p),
        )

    def start_both(make, *args):
        @pl.when(has_up)
        def _():
            make(*args, 0).start()

        @pl.when(has_down)
        def _():
            make(*args, 1).start()

    def wait_recv_both(make, *args):
        @pl.when(has_up)
        def _():
            make(*args, 1).wait_recv()

        @pl.when(has_down)
        def _():
            make(*args, 0).wait_recv()

    pl.semaphore_wait(barrier, 9)
    for j in range(pairs):
        start_both(halo_copy, 0, j)

    pltpu.make_async_copy(g_in, g_in, in_sem.at[1]).wait()
    order = order_ref[...]

    def extended_row(base, count):
        return lax.broadcasted_iota(jnp.int32, (count, 1), 0) + base

    for blk in range(4):
        if blk < 2:
            rows = extended_row(256 + 256 * blk, 256)
        elif blk == 2:
            rows = jnp.concatenate(
                [extended_row(b + 16 * q, 16) for q in range(8) for b in (128, 768)], axis=0
            )
        else:
            rows = jnp.concatenate([extended_row(0, 128), extended_row(896, 128)], axis=0)
        hot = jnp.where(rows == order, 1.0, 0.0).astype(BF16)
        at = 256 * blk
        for m in range(2):
            r0 = 384 * m
            re = lax.dot_general(
                g_in[r0 : r0 + 384, 0:1024], hot, (((1,), (1,)), ((), ())), preferred_element_type=F32
            )
            im = lax.dot_general(
                g_in[r0 : r0 + 384, 1024:2048], hot, (((1,), (1,)), ((), ())), preferred_element_type=F32
            )
            gp[r0 : r0 + 384, at : at + 256] = rounded(re)
            gp[768 + r0 : 768 + r0 + 384, at : at + 256] = rounded(im)

    def own_sweep(t, j):
        y = jnp.dot(gp[:, 0:768], e1[t, j, 0:768, :], preferred_element_type=F32)
        for i in range(2):
            for d in range(2):
                x[2 * j + i, d, 8:776, :] = y[768 * d : 768 * d + 768, N * i : N * i + N]

    def margin_sweep(t, j):
        y = jnp.dot(gp[:, 768:1024], e1[t, j, 768:1024, :], preferred_element_type=F32)
        for i in range(2):
            for d in range(2):
                x[2 * j + i, d, 8:776, :] += y[768 * d : 768 * d + 768, N * i : N * i + N]

    def residual(t, c):
        for b in (0, 5, 1, 2, 3, 4):
            at = 8 + 128 * b

            def lap(d):
                v = (
                    4.0 * x[c, d, at : at + 128, :]
                    - x[c, d, at - 1 : at + 127, :]
                    - x[c, d, at + 1 : at + 129, :]
                )
                if b > 0:
                    v = v - x[c, d, at - 128 : at, :]
                if b < 5:
                    v = v - x[c, d, at + 128 : at + 256, :]
                return v

            xr = x[c, 0, at : at + 128, :]
            xi = x[c, 1, at : at + 128, :]
            sigma = cb[128 * b : 128 * b + 128, :]
            src = st[c, 128 * b : 128 * b + 128, :]
            rr = src - lap(0) - sigma * (shift_re * xr - shift_im * xi)
            ri = -lap(1) - sigma * (shift_im * xr + shift_re * xi)
            acc[c, 128 * b : 128 * b + 128, :] = w_re * xr - w_im * xi
            if 0 < b < 5:
                e2[c, 128 * (b - 1) : 128 * b, 0:N] = rounded(rr)
                e2[c, 128 * (b - 1) : 128 * b, N : 2 * N] = rounded(ri)
            else:
                d = 0 if b == 0 else 1
                rp[c, d, 0] = rr
                rp[c, d, 1] = ri
                for i, v in enumerate((xr, xi, rr, ri)):
                    peak = peak_of(v)
                    p1sp[d, t, c, i : i + 1, :] = peak
                    p1s[d, t, c, i] = coded(v, peak)
        start_both(edge_copy, t, c)

    def weighted(y):
        re = y[:768, 0:N] - y[768:, N : 2 * N]
        im = y[:768, N : 2 * N] + y[768:, 0:N]
        return w_re * re - w_im * im

    def inner_product(c, _):
        acc[c] += weighted(jnp.dot(gp[:, 0:512], e2[c, 0:512, :], preferred_element_type=F32))
        return 0

    row_of = lax.broadcasted_iota(jnp.int32, (H, 1), 0)
    up_on = jnp.where(has_up, 1.0, 0.0).astype(F32)
    down_on = jnp.where(has_down, 1.0, 0.0).astype(F32)

    def rs_copy(t, c, k):
        q = pole_at(*PEERS[k])
        return Several(
            remote(rssp.at[t, c], rsrp.at[t, c, k], rs_ss.at[1], rs_rs.at[t, c, 1], s, q),
            remote(rss.at[t, c, q], rsr.at[t, c, k], rs_ss.at[0], rs_rs.at[t, c, 0], s, q),
        )

    def finish(t, c):
        wait_recv_both(edge_copy, t, c)
        for d in range(2):
            base = 512
            to = slice(N * d, N * d + N)

            def came(side, i):
                return decoded(p1r[side, t, c, i], p1rp[side, t, c, i : i + 1, :])

            above, below = came(0, d), came(1, d)
            top = rp[c, 0, d] + above + jnp.where(row_of == 0, above[127:128], 0.0)
            bottom = rp[c, 1, d] + below + jnp.where(row_of == 127, below[0:1], 0.0)
            top, bottom = rounded(top), rounded(bottom)
            for q in range(8):
                e2[c, base + 32 * q : base + 32 * q + 16, to] = top[16 * q : 16 * q + 16]
                e2[c, base + 32 * q + 16 : base + 32 * q + 32, to] = bottom[16 * q : 16 * q + 16]
            first = x[c, d, 8:136, :]
            final = x[c, d, 648:776, :]
            over = came(0, 2 + d) + first + jnp.where(row_of == 127, first[0:1], 0.0)
            under = came(1, 2 + d) + final + jnp.where(row_of == 0, final[127:128], 0.0)
            e2[c, base + 256 : base + 384, to] = rounded(up_on * over)
            e2[c, base + 384 : base + 512, to] = rounded(down_on * under)
        total = acc[c] + weighted(jnp.dot(gp[:, 512:1024], e2[c, 512:1024, :], preferred_element_type=F32))
        peak = peak_of(total)
        rssp[t, c] = peak
        total = coded(total, peak)
        for q in range(8):
            if t == 0:
                rss[t, c, q, 0:64, :] = total[128 + 64 * q : 192 + 64 * q]
                rss[t, c, q, 64:80, :] = total[16 * q : 16 * q + 16]
                rss[t, c, q, 80:96, :] = total[640 + 16 * q : 656 + 16 * q]
            else:
                rss[t, c, q] = total[96 * q : 96 * q + 96]
        for k in range(7):
            rs_copy(t, c, k).start()

    def all_came(ref, sem):
        pltpu.make_async_copy(ref, ref, sem).wait()

    def summed(t, c):
        total = decoded(rss[t, c, p], rssp[t, c])
        all_came(rsrp.at[t, c], rs_rs.at[t, c, 1])
        all_came(rsr.at[t, c], rs_rs.at[t, c, 0])
        for k in range(7):
            total = total + decoded(rsr[t, c, k], rsrp[t, c, k])
        return total

    def ag_copy(c, k, part):
        q = pole_at(*PEERS[k])
        if part:
            return remote(ags.at[c, pl.ds(0, 64)], agm.at[c, k], ag_ss.at[0], ag_rs.at[c, 0], s, q)
        return Several(
            remote(agsp.at[c], agrp.at[c, k], ag_ss.at[2], ag_rs.at[c, 2], s, q),
            remote(ags.at[c, pl.ds(64, 32)], age.at[c, k], ag_ss.at[1], ag_rs.at[c, 1], s, q),
        )

    def placed_middle(j, i, q, share):
        to = slice(N * i, N * i + N)
        st[2 * j + i, pl.ds(pl.multiple_of(128 + 64 * q, 64), 64), :] = share
        e1[1, j, pl.ds(pl.multiple_of(64 * q, 64), 64), to] = rounded(share)

    def placed_edges(j, i, q, share):
        c, to = 2 * j + i, slice(N * i, N * i + N)
        st[c, pl.ds(pl.multiple_of(16 * q, 16), 16), :] = share[0:16]
        st[c, pl.ds(pl.multiple_of(640 + 16 * q, 16), 16), :] = share[16:32]
        share = rounded(share)
        e1[1, j, pl.ds(pl.multiple_of(512 + 32 * q, 32), 32), to] = share

        @pl.when(j < pairs - 1)
        def _():
            hs[0, pairs + j, pl.ds(pl.multiple_of(16 * q, 16), 16), to] = share[0:16]
            hs[1, pairs + j, pl.ds(pl.multiple_of(16 * q, 16), 16), to] = share[16:32]

    last = pairs - 1

    def margin_copy(i, k, d):
        dst = e1.at[1, last, pl.ds(pl.multiple_of(896 - 128 * d + 16 * p, 16), 16), pl.ds(N * i, N)]
        return remote(
            nbs.at[i, d], dst, nb_ss.at[d], nb_rs.at[i, d], down if d else up, pole_at(*EVERY[k])
        )

    def margins_of(i, edges):
        for d in range(2):
            nbs[i, d] = edges[16 * d : 16 * d + 16]

        @pl.when(has_up)
        def _():
            for k in range(8):
                margin_copy(i, k, 0).start()

        @pl.when(has_down)
        def _():
            for k in range(8):
                margin_copy(i, k, 1).start()

    def margins_in():
        for i in range(2):
            to = pl.ds(N * i, N)

            @pl.when(has_up)
            def _():
                all_came(e1.at[1, last, pl.ds(768, H), to], nb_rs.at[i, 1])

            @pl.when(has_down)
            def _():
                all_came(e1.at[1, last, pl.ds(896, H), to], nb_rs.at[i, 0])

    def next_source(j, i):
        c = 2 * j + i
        total = summed(0, c)
        sigma = jnp.concatenate(
            [
                cb[pl.ds(pl.multiple_of(128 + 64 * p, 64), 64), :],
                cb[pl.ds(pl.multiple_of(16 * p, 16), 16), :],
                cb[pl.ds(pl.multiple_of(640 + 16 * p, 16), 16), :],
            ],
            axis=0,
        )
        share = sigma * total
        peak = peak_of(share)
        agsp[c] = peak
        ags[c] = coded(share, peak)
        for k in range(7):
            ag_copy(c, k, 0).start()

        @pl.when(j == last)
        def _():
            margins_of(i, rounded(share[64:96]))

        for k in range(7):
            ag_copy(c, k, 1).start()
        placed_middle(j, i, p, share[0:64])
        placed_edges(j, i, p, share[64:96])

    def edges_in(j):
        for i in range(2):
            c = 2 * j + i
            all_came(agrp.at[c], ag_rs.at[c, 2])
            all_came(age.at[c], ag_rs.at[c, 1])
            for k, (dx, dz) in enumerate(PEERS):
                placed_edges(j, i, pole_at(4 - dx, dz), decoded(age[c, k], agrp[c, k]))

        @pl.when(j < last)
        def _():
            start_both(halo_copy, 1, j)

    def middle_in(j):
        for i in range(2):
            c = 2 * j + i
            all_came(agm.at[c], ag_rs.at[c, 0])
            for k, (dx, dz) in enumerate(PEERS):
                placed_middle(j, i, pole_at(4 - dx, dz), decoded(agm[c, k], agrp[c, k]))

    def over_pairs(step, *args):
        def body(j, _):
            step(*args, j)
            return 0

        lax.fori_loop(0, pairs, body, 0)

    def first_sweep(t, j):
        if t == 0:
            wait_recv_both(halo_copy, t, j)
        else:

            @pl.when(j < last)
            def _():
                wait_recv_both(halo_copy, 1, j)

            @pl.when(j == last)
            def _():
                margins_in()

        margin_sweep(t, j)

        def body(i, _):
            residual(t, 2 * j + i)
            return 0

        lax.fori_loop(0, 2, body, 0)

    def opening(j):
        own_sweep(0, j)
        first_sweep(0, j)

    def opening_again(j):
        middle_in(j)
        own_sweep(1, j)

        @pl.when(j + 1 < pairs)
        def _():
            edges_in(j + 1)

        first_sweep(1, j)

    def both_next(j):
        for i in range(2):
            next_source(j, i)

    def second_sweep(t):
        def rest(c):
            @pl.when(c < chunks - 2)
            def _():
                inner_product(c + 2, 0)

        def body(c, _):
            if t == 1:
                rest(c)
            finish(t, c)
            if t == 0:
                rest(c)
            return 0

        lax.fori_loop(0, chunks, body, 0)

    def both_of(step, j):
        step(j)

        @pl.when(j == 0)
        def _():
            lax.fori_loop(0, 2, inner_product, 0)

    over_pairs(both_of, opening)
    second_sweep(0)
    over_pairs(both_next)
    edges_in(0)
    over_pairs(both_of, opening_again)
    second_sweep(1)

    for c in range(chunks):
        res[:, c * N : c * N + N] = summed(1, c)
        pltpu.make_async_copy(
            res.at[:, pl.ds(c * N, N)], out_ref.at[:, pl.ds(c * N, N)], in_sem.at[0]
        ).start()

    all_came(rsr, rs_ss.at[0])
    all_came(rsrp, rs_ss.at[1])
    all_came(agm, ag_ss.at[0])
    all_came(age, ag_ss.at[1])
    all_came(agrp, ag_ss.at[2])

    def all_left(d):
        all_came(hs.at[d], halo_ss.at[d])
        all_came(e1.at[0, 0, pl.ds(0, 256), pl.ds(0, N)], nb_ss.at[d])
        all_came(p1s.at[d], p1_ss.at[d, 0])
        all_came(p1sp.at[d], p1_ss.at[d, 1])

    @pl.when(has_up)
    def _():
        all_left(0)

    @pl.when(has_down)
    def _():
        all_left(1)

    all_came(res, in_sem.at[0])


def shards(state, conductivity, pole_shift, pole_weight, order_list, inverse):
    rows, columns = state.shape
    chunks = columns // N
    vmem = pl.BlockSpec(memory_space=pltpu.VMEM)
    smem = pl.BlockSpec(memory_space=pltpu.SMEM)
    anywhere = pl.BlockSpec(memory_space=pl.ANY)
    hbm = pl.BlockSpec(memory_space=pltpu.HBM)
    dma = pltpu.SemaphoreType.DMA

    def body(*refs):
        kernel(chunks, *refs)

    return pl.pallas_call(
        body,
        out_shape=jax.ShapeDtypeStruct((rows // 8, columns), F32),
        in_specs=[vmem, vmem, smem, smem, hbm, hbm],
        out_specs=anywhere,
        scratch_shapes=[
            pltpu.VMEM((768, 2048), BF16),
            pltpu.VMEM((chunks, 768, N), F32),
            pltpu.VMEM((768, N), F32),
            pltpu.VMEM((1536, 1024), BF16),
            pltpu.VMEM((2, chunks // 2, 1024, PAIR), BF16),
            pltpu.VMEM((2, 2 * (chunks // 2) - 1, H, PAIR), BF16),
            pltpu.VMEM((chunks, 2, 784, N), F32),
            pltpu.VMEM((chunks, 768, N), F32),
            pltpu.VMEM((chunks, 2, 2, H, N), F32),
            pltpu.VMEM((2, 2, chunks, 4, H, N), I16),
            pltpu.VMEM((2, 2, chunks, 4, H, N), I16),
            pltpu.VMEM((2, 2, chunks, 4, N), F32),
            pltpu.VMEM((2, 2, chunks, 4, N), F32),
            pltpu.VMEM((chunks, 1024, 2 * N), BF16),
            pltpu.VMEM((2, chunks, 8, 96, N), I16),
            pltpu.VMEM((2, chunks, 7, 96, N), I16),
            pltpu.VMEM((2, chunks, 1, N), F32),
            pltpu.VMEM((2, chunks, 7, 1, N), F32),
            pltpu.VMEM((chunks, 96, N), I16),
            pltpu.VMEM((chunks, 7, 64, N), I16),
            pltpu.VMEM((chunks, 7, 32, N), I16),
            pltpu.VMEM((chunks, 1, N), F32),
            pltpu.VMEM((chunks, 7, 1, N), F32),
            pltpu.VMEM((2, 2, 16, N), BF16),
            pltpu.VMEM((96, chunks * N), F32),
            dma((2,)),
            dma((2,)),
            dma((2, chunks // 2, 2)),
            dma((2, 2)),
            dma((2, chunks, 2, 2)),
            dma((2,)),
            dma((2, chunks, 2)),
            dma((3,)),
            dma((chunks, 3)),
            dma((2,)),
            dma((2, 2)),
        ],
        compiler_params=pltpu.CompilerParams(
            collective_id=0, has_side_effects=True, vmem_limit_bytes=58 << 20
        ),
    )(order_list, conductivity, pole_shift, pole_weight, state, inverse)


def solution(mesh):
    placed = (
        P("sub", None),
        P("sub"),
        P("pole", None),
        P("pole", None),
        P("sub", None),
        P("pole", "sub", None),
    )
    return jax.shard_map(
        shards, mesh=mesh, in_specs=placed, out_specs=P(("sub", "pole"), None), check_vma=False
    )
```

```python
import jax
import jax.numpy as jnp
from jax import lax
from jax.experimental import pallas as pl
from jax.experimental.pallas import tpu as pltpu
from jax.sharding import PartitionSpec as P

MESH = pl.DeviceIdType.MESH
F32 = jnp.float32
BF16 = jnp.bfloat16
H = 128
N = 128
PAIR = 2 * N
PEERS = ((2, 1), (0, 1), (2, 0), (1, 1), (3, 1), (1, 0), (3, 0))
I16 = jnp.int16
TOP = 32767.0


def rounded(x):
    return x.astype(BF16)


def coded(v, peak):
    return jnp.round(v * (TOP / peak)).astype(jnp.int32).astype(I16)


def peak_of(v):
    return jnp.maximum(jnp.max(jnp.abs(v), axis=0, keepdims=True), 1e-30)


def decoded(q, peak):
    return q.astype(jnp.int32).astype(F32) * (peak * (1.0 / TOP))


def kernel(
    chunks, order_ref, cond_ref, shift_ref, weight_ref, state_hbm, inv_hbm, out_ref,
    g_in, st, cb, gp, e1, hs, x, acc, rp, p1s, p1r, p1sp, p1rp, e2, rss, rsr, rssp, rsrp,
    ags, agr, agsp, agrp, res,
    in_sem, halo_ss, halo_rs, p1_ss, p1_rs, rs_ss, rs_rs, ag_ss, ag_rs,
):
    pairs = chunks // 2
    s = lax.axis_index("sub")
    p = lax.axis_index("pole")
    px, pz = p // 2, lax.rem(p, 2)
    subs = lax.axis_size("sub")
    has_up, has_down = s > 0, s < subs - 1
    up, down = lax.rem(s + subs - 1, subs), lax.rem(s + 1, subs)

    def pole_at(dx, dz):
        return lax.rem(px + dx, 4) * 2 + lax.rem(pz + dz, 2)

    def remote(src, dst, send_sem, recv_sem, sub, pole):
        return pltpu.make_async_remote_copy(
            src_ref=src, dst_ref=dst, send_sem=send_sem, recv_sem=recv_sem,
            device_id=(sub, pole), device_id_type=MESH,
        )

    state_in = [
        pltpu.make_async_copy(state_hbm.at[:, pl.ds(c * N, N)], st.at[c], in_sem.at[0])
        for c in range(chunks)
    ]
    for copy in state_in:
        copy.start()
    g_copy = pltpu.make_async_copy(inv_hbm.at[0], g_in, in_sem.at[1])
    g_copy.start()

    barrier = pltpu.get_barrier_semaphore()
    for dx, dz in PEERS:
        pl.semaphore_signal(barrier, inc=1, device_id=(s, pole_at(dx, dz)), device_id_type=MESH)
    pl.semaphore_signal(barrier, inc=1, device_id=(up, p), device_id_type=MESH)
    pl.semaphore_signal(barrier, inc=1, device_id=(down, p), device_id_type=MESH)

    shift_re, shift_im = shift_ref[0, 0], shift_ref[0, 1]
    w_re, w_im = 2.0 * weight_ref[0, 0], 2.0 * weight_ref[0, 1]

    for b in range(6):
        row = cond_ref[128 * b : 128 * b + 128]
        cb[128 * b : 128 * b + 128, :] = jnp.broadcast_to(row[None, :], (128, 128)).T

    for c in range(chunks):
        for d in range(2):
            x[c, d, 0:8, :] = jnp.zeros((8, N), F32)
            x[c, d, 776:784, :] = jnp.zeros((8, N), F32)

    @pl.when(jnp.logical_not(has_up))
    def _():
        for t in range(2):
            for j in range(pairs):
                e1[t, j, 768:896, :] = jnp.zeros((H, PAIR), BF16)
            for c in range(chunks):
                p1r[0, t, c] = jnp.zeros((4, H, N), I16)
                p1rp[0, t, c] = jnp.zeros((4, N), F32)

    @pl.when(jnp.logical_not(has_down))
    def _():
        for t in range(2):
            for j in range(pairs):
                e1[t, j, 896:1024, :] = jnp.zeros((H, PAIR), BF16)
            for c in range(chunks):
                p1r[1, t, c] = jnp.zeros((4, H, N), I16)
                p1rp[1, t, c] = jnp.zeros((4, N), F32)

    pltpu.make_async_copy(st, st, in_sem.at[0]).wait()
    for c in range(chunks):
        j, to = c // 2, slice(N * (c % 2), N * (c % 2) + N)
        src = cb[...] * st[c]
        st[c] = src
        e1[0, j, 0:512, to] = rounded(src[128:640])
        top = rounded(src[0:128])
        bottom = rounded(src[640:768])
        hs[0, 0, j, :, to] = top
        hs[1, 0, j, :, to] = bottom
        for q in range(8):
            e1[0, j, 512 + 32 * q : 528 + 32 * q, to] = top[16 * q : 16 * q + 16]
            e1[0, j, 528 + 32 * q : 544 + 32 * q, to] = bottom[16 * q : 16 * q + 16]

    def halo_copy(t, j, d):
        return remote(
            hs.at[d, t, j], e1.at[t, j, pl.ds(896 - 128 * d, H)], halo_ss.at[d], halo_rs.at[t, j, d],
            down if d else up, p,
        )

    class Several:
        def __init__(self, *copies):
            self.copies = copies

        def start(self):
            for copy in self.copies:
                copy.start()

        def wait_recv(self):
            for copy in self.copies:
                copy.wait_recv()

        def wait_send(self):
            for copy in self.copies:
                copy.wait_send()

    def edge_copy(t, c, d):
        to = down if d else up
        return Several(
            remote(p1sp.at[d, t, c], p1rp.at[1 - d, t, c], p1_ss.at[d, 1], p1_rs.at[t, c, d, 1], to, p),
            remote(p1s.at[d, t, c], p1r.at[1 - d, t, c], p1_ss.at[d, 0], p1_rs.at[t, c, d, 0], to, p),
        )

    def start_both(make, *args):
        @pl.when(has_up)
        def _():
            make(*args, 0).start()

        @pl.when(has_down)
        def _():
            make(*args, 1).start()

    def wait_recv_both(make, *args):
        @pl.when(has_up)
        def _():
            make(*args, 1).wait_recv()

        @pl.when(has_down)
        def _():
            make(*args, 0).wait_recv()

    g_copy.wait()
    order = order_ref[...]

    def extended_row(base, count):
        return lax.broadcasted_iota(jnp.int32, (count, 1), 0) + base

    for blk in range(4):
        if blk == 2:
            pl.semaphore_wait(barrier, 9)
            for j in range(pairs):
                start_both(halo_copy, 0, j)
        if blk < 2:
            rows = extended_row(256 + 256 * blk, 256)
        elif blk == 2:
            rows = jnp.concatenate(
                [extended_row(b + 16 * q, 16) for q in range(8) for b in (128, 768)], axis=0
            )
        else:
            rows = jnp.concatenate([extended_row(0, 128), extended_row(896, 128)], axis=0)
        hot = jnp.where(rows == order, 1.0, 0.0).astype(BF16)
        at = 256 * blk
        for m in range(2):
            r0 = 384 * m
            re = lax.dot_general(
                g_in[r0 : r0 + 384, 0:1024], hot, (((1,), (1,)), ((), ())), preferred_element_type=F32
            )
            im = lax.dot_general(
                g_in[r0 : r0 + 384, 1024:2048], hot, (((1,), (1,)), ((), ())), preferred_element_type=F32
            )
            gp[r0 : r0 + 384, at : at + 256] = rounded(re)
            gp[768 + r0 : 768 + r0 + 384, at : at + 256] = rounded(im)

    def own_sweep(t, j):
        y = jnp.dot(gp[:, 0:768], e1[t, j, 0:768, :], preferred_element_type=F32)
        for i in range(2):
            for d in range(2):
                x[2 * j + i, d, 8:776, :] = y[768 * d : 768 * d + 768, N * i : N * i + N]

    def margin_sweep(t, j):
        y = jnp.dot(gp[:, 768:1024], e1[t, j, 768:1024, :], preferred_element_type=F32)
        for i in range(2):
            for d in range(2):
                x[2 * j + i, d, 8:776, :] += y[768 * d : 768 * d + 768, N * i : N * i + N]

    def residual(t, c):
        for b in (0, 5, 1, 2, 3, 4):
            at = 8 + 128 * b

            def lap(d):
                v = (
                    4.0 * x[c, d, at : at + 128, :]
                    - x[c, d, at - 1 : at + 127, :]
                    - x[c, d, at + 1 : at + 129, :]
                )
                if b > 0:
                    v = v - x[c, d, at - 128 : at, :]
                if b < 5:
                    v = v - x[c, d, at + 128 : at + 256, :]
                return v

            xr = x[c, 0, at : at + 128, :]
            xi = x[c, 1, at : at + 128, :]
            sigma = cb[128 * b : 128 * b + 128, :]
            src = st[c, 128 * b : 128 * b + 128, :]
            rr = src - lap(0) - sigma * (shift_re * xr - shift_im * xi)
            ri = -lap(1) - sigma * (shift_im * xr + shift_re * xi)
            acc[c, 128 * b : 128 * b + 128, :] = w_re * xr - w_im * xi
            if 0 < b < 5:
                e2[c, 128 * (b - 1) : 128 * b, 0:N] = rounded(rr)
                e2[c, 128 * (b - 1) : 128 * b, N : 2 * N] = rounded(ri)
            else:
                d = 0 if b == 0 else 1
                rp[c, d, 0] = rr
                rp[c, d, 1] = ri
                for i, v in enumerate((xr, xi, rr, ri)):
                    peak = peak_of(v)
                    p1sp[d, t, c, i : i + 1, :] = peak
                    p1s[d, t, c, i] = coded(v, peak)
            if b == 5:
                start_both(edge_copy, t, c)

    def weighted(y):
        re = y[:768, 0:N] - y[768:, N : 2 * N]
        im = y[:768, N : 2 * N] + y[768:, 0:N]
        return w_re * re - w_im * im

    def inner_product(c, _):
        acc[c] += weighted(jnp.dot(gp[:, 0:512], e2[c, 0:512, :], preferred_element_type=F32))
        return 0

    row_of = lax.broadcasted_iota(jnp.int32, (H, 1), 0)
    up_on = jnp.where(has_up, 1.0, 0.0).astype(F32)
    down_on = jnp.where(has_down, 1.0, 0.0).astype(F32)

    def rs_copy(t, c, k):
        q = pole_at(*PEERS[k])
        return Several(
            remote(rssp.at[t, c], rsrp.at[t, c, k], rs_ss.at[1], rs_rs.at[t, c, 1], s, q),
            remote(rss.at[t, c, q], rsr.at[t, c, k], rs_ss.at[0], rs_rs.at[t, c, 0], s, q),
        )

    def finish(t, c):
        wait_recv_both(edge_copy, t, c)
        for d in range(2):
            base = 512
            to = slice(N * d, N * d + N)

            def came(side, i):
                return decoded(p1r[side, t, c, i], p1rp[side, t, c, i : i + 1, :])

            above, below = came(0, d), came(1, d)
            top = rp[c, 0, d] + above + jnp.where(row_of == 0, above[127:128], 0.0)
            bottom = rp[c, 1, d] + below + jnp.where(row_of == 127, below[0:1], 0.0)
            top, bottom = rounded(top), rounded(bottom)
            for q in range(8):
                e2[c, base + 32 * q : base + 32 * q + 16, to] = top[16 * q : 16 * q + 16]
                e2[c, base + 32 * q + 16 : base + 32 * q + 32, to] = bottom[16 * q : 16 * q + 16]
            first = x[c, d, 8:136, :]
            final = x[c, d, 648:776, :]
            over = came(0, 2 + d) + first + jnp.where(row_of == 127, first[0:1], 0.0)
            under = came(1, 2 + d) + final + jnp.where(row_of == 0, final[127:128], 0.0)
            e2[c, base + 256 : base + 384, to] = rounded(up_on * over)
            e2[c, base + 384 : base + 512, to] = rounded(down_on * under)
        total = acc[c] + weighted(jnp.dot(gp[:, 512:1024], e2[c, 512:1024, :], preferred_element_type=F32))
        peak = peak_of(total)
        rssp[t, c] = peak
        total = coded(total, peak)
        for q in range(8):
            if t == 0:
                rss[t, c, q, 0:64, :] = total[128 + 64 * q : 192 + 64 * q]
                rss[t, c, q, 64:80, :] = total[16 * q : 16 * q + 16]
                rss[t, c, q, 80:96, :] = total[640 + 16 * q : 656 + 16 * q]
            else:
                rss[t, c, q] = total[96 * q : 96 * q + 96]
        for k in range(7):
            rs_copy(t, c, k).start()

    def all_came(ref, sem):
        pltpu.make_async_copy(ref, ref, sem).wait()

    def summed(t, c):
        total = decoded(rss[t, c, p], rssp[t, c])
        all_came(rsrp.at[t, c], rs_rs.at[t, c, 1])
        all_came(rsr.at[t, c], rs_rs.at[t, c, 0])
        for k in range(7):
            total = total + decoded(rsr[t, c, k], rsrp[t, c, k])
        return total

    def ag_copy(c, k):
        q = pole_at(*PEERS[k])
        return Several(
            remote(agsp.at[c], agrp.at[c, k], ag_ss.at[1], ag_rs.at[c, 1], s, q),
            remote(ags.at[c], agr.at[c, k], ag_ss.at[0], ag_rs.at[c, 0], s, q),
        )

    def placed_share(j, i, q, share):
        c, to = 2 * j + i, slice(N * i, N * i + N)
        st[c, pl.ds(pl.multiple_of(128 + 64 * q, 64), 64), :] = share[0:64]
        st[c, pl.ds(pl.multiple_of(16 * q, 16), 16), :] = share[64:80]
        st[c, pl.ds(pl.multiple_of(640 + 16 * q, 16), 16), :] = share[80:96]
        share = rounded(share)
        e1[1, j, pl.ds(pl.multiple_of(64 * q, 64), 64), to] = share[0:64]
        e1[1, j, pl.ds(pl.multiple_of(512 + 32 * q, 32), 32), to] = share[64:96]
        hs[0, 1, j, pl.ds(pl.multiple_of(16 * q, 16), 16), to] = share[64:80]
        hs[1, 1, j, pl.ds(pl.multiple_of(16 * q, 16), 16), to] = share[80:96]

    def next_source(j, i):
        c = 2 * j + i
        total = summed(0, c)
        sigma = jnp.concatenate(
            [
                cb[pl.ds(pl.multiple_of(128 + 64 * p, 64), 64), :],
                cb[pl.ds(pl.multiple_of(16 * p, 16), 16), :],
                cb[pl.ds(pl.multiple_of(640 + 16 * p, 16), 16), :],
            ],
            axis=0,
        )
        share = sigma * total
        peak = peak_of(share)
        agsp[c] = peak
        ags[c] = coded(share, peak)
        for k in range(7):
            ag_copy(c, k).start()
        placed_share(j, i, p, share)

    def source_arrived(j):
        for i in range(2):
            c = 2 * j + i
            all_came(agrp.at[c], ag_rs.at[c, 1])
            all_came(agr.at[c], ag_rs.at[c, 0])
            for k, (dx, dz) in enumerate(PEERS):
                placed_share(j, i, pole_at(4 - dx, dz), decoded(agr[c, k], agrp[c, k]))
        start_both(halo_copy, 1, j)

    def over_pairs(step, *args):
        def body(j, _):
            step(*args, j)
            return 0

        lax.fori_loop(0, pairs, body, 0)

    def first_sweep(t, j):
        wait_recv_both(halo_copy, t, j)
        margin_sweep(t, j)

        def body(i, _):
            residual(t, 2 * j + i)
            return 0

        lax.fori_loop(0, 2, body, 0)

    def second_sweep(t):
        def body(c, _):
            finish(t, c)
            return 0

        lax.fori_loop(0, chunks, inner_product, 0)
        lax.fori_loop(0, chunks, body, 0)

    def both_next(j):
        for i in range(2):
            next_source(j, i)

    def source_in(j):
        source_arrived(j)
        own_sweep(1, j)

    over_pairs(own_sweep, 0)
    over_pairs(first_sweep, 0)
    second_sweep(0)
    over_pairs(both_next)
    over_pairs(source_in)
    over_pairs(first_sweep, 1)
    second_sweep(1)

    for c in range(chunks):
        res[:, c * N : c * N + N] = summed(1, c)
        pltpu.make_async_copy(
            res.at[:, pl.ds(c * N, N)], out_ref.at[:, pl.ds(c * N, N)], in_sem.at[0]
        ).start()

    all_came(rsr, rs_ss.at[0])
    all_came(rsrp, rs_ss.at[1])
    all_came(agr, ag_ss.at[0])
    all_came(agrp, ag_ss.at[1])

    def all_left(d):
        all_came(hs.at[d], halo_ss.at[d])
        all_came(p1s.at[d], p1_ss.at[d, 0])
        all_came(p1sp.at[d], p1_ss.at[d, 1])

    @pl.when(has_up)
    def _():
        all_left(0)

    @pl.when(has_down)
    def _():
        all_left(1)

    all_came(res, in_sem.at[0])


def shards(state, conductivity, pole_shift, pole_weight, order_list, inverse):
    rows, columns = state.shape
    chunks = columns // N
    vmem = pl.BlockSpec(memory_space=pltpu.VMEM)
    smem = pl.BlockSpec(memory_space=pltpu.SMEM)
    anywhere = pl.BlockSpec(memory_space=pl.ANY)
    dma = pltpu.SemaphoreType.DMA

    def body(*refs):
        kernel(chunks, *refs)

    return pl.pallas_call(
        body,
        out_shape=jax.ShapeDtypeStruct((rows // 8, columns), F32),
        in_specs=[vmem, vmem, smem, smem, anywhere, anywhere],
        out_specs=anywhere,
        scratch_shapes=[
            pltpu.VMEM((768, 2048), BF16),
            pltpu.VMEM((chunks, 768, N), F32),
            pltpu.VMEM((768, N), F32),
            pltpu.VMEM((1536, 1024), BF16),
            pltpu.VMEM((2, chunks // 2, 1024, PAIR), BF16),
            pltpu.VMEM((2, 2, chunks // 2, H, PAIR), BF16),
            pltpu.VMEM((chunks, 2, 784, N), F32),
            pltpu.VMEM((chunks, 768, N), F32),
            pltpu.VMEM((chunks, 2, 2, H, N), F32),
            pltpu.VMEM((2, 2, chunks, 4, H, N), I16),
            pltpu.VMEM((2, 2, chunks, 4, H, N), I16),
            pltpu.VMEM((2, 2, chunks, 4, N), F32),
            pltpu.VMEM((2, 2, chunks, 4, N), F32),
            pltpu.VMEM((chunks, 1024, 2 * N), BF16),
            pltpu.VMEM((2, chunks, 8, 96, N), I16),
            pltpu.VMEM((2, chunks, 7, 96, N), I16),
            pltpu.VMEM((2, chunks, 1, N), F32),
            pltpu.VMEM((2, chunks, 7, 1, N), F32),
            pltpu.VMEM((chunks, 96, N), I16),
            pltpu.VMEM((chunks, 7, 96, N), I16),
            pltpu.VMEM((chunks, 1, N), F32),
            pltpu.VMEM((chunks, 7, 1, N), F32),
            pltpu.VMEM((96, chunks * N), F32),
            dma((2,)),
            dma((2,)),
            dma((2, chunks // 2, 2)),
            dma((2, 2)),
            dma((2, chunks, 2, 2)),
            dma((2,)),
            dma((2, chunks, 2)),
            dma((2,)),
            dma((chunks, 2)),
        ],
        compiler_params=pltpu.CompilerParams(
            collective_id=0, has_side_effects=True, vmem_limit_bytes=58 << 20
        ),
    )(order_list, conductivity, pole_shift, pole_weight, state, inverse)


def solution(mesh):
    placed = (
        P("sub", None),
        P("sub"),
        P("pole", None),
        P("pole", None),
        P("sub", None),
        P("pole", "sub", None),
    )
    return jax.shard_map(
        shards, mesh=mesh, in_specs=placed, out_specs=P(("sub", "pole"), None), check_vma=False
    )
```
